256 devices in a mesh: rows: 16 (over y, x), tp: 16 (over z, core).
Axes of the slice: x: 4, y: 4, z: 8, core: 2. Of those that a mesh axis runs over, the one named last changes fastest.
Arguments:
- train_gate: float32 [3584, 14336], P('rows', 'tp'), may hold values from -0.125 to 0.125
- drift_gate: float32 [3584, 14336], P('rows', 'tp'), may hold values from -6 to 6
- spread_gate: float32 [3584, 14336], P('rows', 'tp'), may hold values from 0.1 to 10
- train_up: float32 [3584, 14336], P('rows', 'tp'), may hold values from -0.125 to 0.125
- drift_up: float32 [3584, 14336], P('rows', 'tp'), may hold values from -6 to 6
- spread_up: float32 [3584, 14336], P('rows', 'tp'), may hold values from 0.1 to 10
- norm_gain: float32 [3584], P('rows'), may hold values from 0.25 to 1.75
Outputs:
- serving_gate: bfloat16 [3584, 14336], P(None, 'tp')
- serving_up: bfloat16 [3584, 14336], P(None, 'tp')
- column_gate: float32 [14336], P('tp')
- column_up: float32 [14336], P('tp')
The draws below stay inside these ranges and needn't reach their ends.
All inputs are finite; a program needn't handle non-finite values. Where the reference program divides by a largest or mean magnitude, that divisor is 1e-20 or more.
Results may differ from the reference program's by a relative error of at most 0.001.
Values may be sent and summed in bfloat16 or wider, within the bound.
No kernel may reach another device: no remote copies, remote signals or barrier semaphores. Data moves between devices by JAX's collectives and lax.ppermute only.
A program may use at most 128 MiB of HBM per device.

```python
import math
import jax
import jax.numpy as jnp
from jax import lax

D_MODEL = 3584
D_INNER = 14336


def strengthened(values, rng, source, target, shards_of, factor):
    owner, partner = [(jnp.arange(values.shape[dim]) // (values.shape[dim] // shards_of)).reshape([-1 if axis == dim else 1 for axis in range(values.ndim)]) for dim in (source, target)]
    chosen = jax.random.permutation(rng, shards_of)[partner]
    strong = (owner == chosen) | (owner == (partner + shards_of // 2) % shards_of)
    return jnp.where(strong, factor * values, values)


def steps_of(own_key, shape, shards, low, high):
    def one(axis_at, parts):
        draws = jax.random.uniform(jax.random.fold_in(jax.random.fold_in(own_key, 6), axis_at), (parts,), jnp.float32, low / len(shards), high / len(shards))
        return jnp.repeat(jnp.exp(draws), shape[axis_at] // parts).reshape((-1,) + (1,) * (len(shape) - axis_at - 1))

    gain = one(*shards[0])
    for cut in shards[1:]:
        gain = gain * one(*cut)
    return gain


def bell_draw(own_key, shape, deviation, bound, split=(), dtype=jnp.bfloat16):
    gain = steps_of(own_key, shape, split, -0.22, 0.18) if split else 1.0
    drawn = jax.random.normal(own_key, shape, jnp.float32) * deviation * gain
    return jnp.minimum(jnp.maximum(drawn, -bound), bound).astype(dtype)


def gaussian_with(rng, extent, width, most, shards, heavy, held_as=jnp.bfloat16):
    drawn = width * jax.random.normal(rng, extent, jnp.float32)
    if shards:
        drawn = drawn * steps_of(rng, extent, shards, -0.22, 0.18)
    return jnp.clip(strengthened(drawn, jax.random.fold_in(rng, 3), *heavy), -most, most).astype(held_as)


def setup_inputs(seed: int = 0) -> dict:
    streams_of = jax.random.split(jax.random.key(seed), 8)
    return {
        "train_gate": gaussian_with(streams_of[0], (D_MODEL, D_INNER), D_MODEL ** -0.5, 0.125, ((0, 16), (1, 16)), (0, 1, 16, 2.0), jnp.float32),
        "drift_gate": bell_draw(streams_of[1], (D_MODEL, D_INNER), 1.0, 6.0, ((0, 16), (1, 16)), jnp.float32),
        "spread_gate": jnp.clip(jnp.exp(math.log(10.0) - 4.6051702 * jax.random.uniform(streams_of[2], (D_MODEL, D_INNER), jnp.float32) ** steps_of(streams_of[2], (D_MODEL, D_INNER), ((0, 16), (1, 16)), -0.2, 0.2)), 0.1, 10.0),
        "train_up": gaussian_with(streams_of[3], (D_MODEL, D_INNER), D_MODEL ** -0.5, 0.125, ((0, 16), (1, 16)), (0, 1, 16, 2.0), jnp.float32),
        "drift_up": bell_draw(streams_of[4], (D_MODEL, D_INNER), 1.0, 6.0, ((0, 16), (1, 16)), jnp.float32),
        "spread_up": jnp.clip(jnp.exp(math.log(10.0) - 4.6051702 * jax.random.uniform(streams_of[5], (D_MODEL, D_INNER), jnp.float32) ** steps_of(streams_of[5], (D_MODEL, D_INNER), ((0, 16), (1, 16)), -0.2, 0.2)), 0.1, 10.0),
        "norm_gain": jnp.clip(1.0 + 0.15 * jax.random.normal(streams_of[6], (D_MODEL,), jnp.float32), 0.25, 1.75),
    }


learn_rate = 0.015
decay_rate = 0.1
tiny_value = 1e-08

def reference(train_gate, drift_gate, spread_gate, train_up, drift_up, spread_up, norm_gain):
    whole_gate = train_gate - learn_rate * (drift_gate / (jnp.sqrt(spread_gate) + tiny_value) + decay_rate * train_gate)
    whole_up = train_up - learn_rate * (drift_up / (jnp.sqrt(spread_up) + tiny_value) + decay_rate * train_up)
    whole_gained_gate = whole_gate * norm_gain[:, None]
    whole_gained_up = whole_up * norm_gain[:, None]
    column_gate = lax.optimization_barrier(jnp.max(jnp.abs(whole_gained_gate), axis=0))
    serving_gate = (whole_gained_gate / column_gate).astype(jnp.bfloat16)
    column_up = lax.optimization_barrier(jnp.max(jnp.abs(whole_gained_up), axis=0))
    serving_up = (whole_gained_up / column_up).astype(jnp.bfloat16)
    return (serving_gate, serving_up, column_gate, column_up)
```

```python
import jax
import jax.numpy as jnp
from jax import lax
from jax.experimental import pallas as pl
from jax.experimental.pallas import tpu as pltpu
from jax.sharding import PartitionSpec as P

learn_rate = 0.015
decay_rate = 0.1
tiny_value = 1e-08
SIDE = 4
TP = 16


def send(value, dy, dx):
    pairs = []
    for y in range(SIDE):
        for x in range(SIDE):
            for t in range(TP):
                s = 1 - 2 * (t % 2)
                to = ((y + s * dy) % SIDE) * SIDE + (x + s * dx) % SIDE
                pairs.append(((y * SIDE + x) * TP + t, to * TP + t))
    return lax.ppermute(value, ("rows", "tp"), pairs)


def place(outs, pieces, extra=()):
    blocks = [p[3] for p in pieces]
    rows = blocks[0].shape[0]

    def body(*refs):
        n = len(blocks)
        ins = refs[2 : 2 + n]
        dst = refs[2 + n + len(extra) : 4 + n + len(extra)]
        sems = refs[-1]
        r = lax.axis_index("rows")
        s = 1 - 2 * (lax.axis_index("tp") % 2)
        y, x = r // SIDE, r % SIDE
        copies = []
        for k, (which, dy, dx, _) in enumerate(pieces):
            at = ((y + s * dy + 2 * SIDE) % SIDE) * SIDE + (x + s * dx + 2 * SIDE) % SIDE
            copies.append(pltpu.make_async_copy(ins[k], dst[which].at[pl.ds(at * rows, rows), :], sems.at[k]))
        for c in copies:
            c.start()
        for c in copies:
            c.wait()

    any_spec = pl.BlockSpec(memory_space=pl.ANY)
    return pl.pallas_call(
        body,
        out_shape=tuple(jax.ShapeDtypeStruct(o.shape, o.dtype) for o in outs),
        in_specs=[any_spec] * (2 + len(blocks) + len(extra)),
        out_specs=(any_spec, any_spec),
        input_output_aliases={0: 0, 1: 1},
        scratch_shapes=[pltpu.SemaphoreType.DMA((len(blocks),))],
    )(*outs, *blocks, *extra)


def blank(shape, dtype):
    return pl.pallas_call(
        lambda a, b: None,
        out_shape=(jax.ShapeDtypeStruct(shape, dtype),) * 2,
        out_specs=(pl.BlockSpec(memory_space=pl.ANY),) * 2,
    )()


def max_over(v):
    c = jnp.broadcast_to(v, (SIDE * SIDE, v.shape[0]))
    return jnp.max(lax.all_to_all(c, "rows", 0, 0, tiled=True), axis=0)


def per_device(train_gate, drift_gate, spread_gate, train_up, drift_up, spread_up, norm_gain):
    whole_gate = train_gate - learn_rate * (
        drift_gate / (jnp.sqrt(spread_gate) + tiny_value) + decay_rate * train_gate
    )
    whole_up = train_up - learn_rate * (
        drift_up / (jnp.sqrt(spread_up) + tiny_value) + decay_rate * train_up
    )
    gained_gate = whole_gate * norm_gain[:, None]
    gained_up = whole_up * norm_gain[:, None]
    both = jnp.concatenate([jnp.max(jnp.abs(gained_gate), axis=0), jnp.max(jnp.abs(gained_up), axis=0)])
    both = max_over(both)
    width = train_gate.shape[1]
    column_gate, column_up = both[:width], both[width:]
    g = (gained_gate / column_gate).astype(jnp.bfloat16)
    u = (gained_up / column_up).astype(jnp.bfloat16)
    outs = blank((train_gate.shape[0] * SIDE * SIDE, width), jnp.bfloat16)

    gx1, uy1, gx2, uy2 = send(g, 0, 1), send(u, 1, 0), send(g, 0, -1), send(u, -1, 0)
    ux1, gy1, ux2, gy2 = send(u, 0, 1), send(g, 1, 0), send(u, 0, -1), send(g, -1, 0)
    gx3, uy3 = send(gx1, 0, 1), send(uy1, 1, 0)
    ux3, gy3 = send(ux2, 0, -1), send(gy2, -1, 0)
    g11, u11, g12, u12 = send(gx1, 1, 0), send(uy1, 0, 1), send(gx1, -1, 0), send(uy1, 0, -1)
    g21, u21, g22, u22 = send(gx2, 1, 0), send(uy2, 0, 1), send(gx2, -1, 0), send(uy2, 0, -1)
    g31, u31, g32, u32 = send(gx3, 1, 0), send(uy3, 0, 1), send(gx3, -1, 0), send(uy3, 0, -1)
    g13, u13 = send(g11, 1, 0), send(u11, 0, 1)
    g23, u23 = send(g22, -1, 0), send(u22, 0, -1)
    g33, u33 = send(g31, 1, 0), send(u31, 0, 1)

    outs = place(outs, [
        (0, 0, 0, g), (1, 0, 0, u),
        (0, 0, -1, gx1), (0, 0, 1, gx2), (1, -1, 0, uy1), (1, 1, 0, uy2),
        (1, 0, -1, ux1), (1, 0, 1, ux2), (0, -1, 0, gy1), (0, 1, 0, gy2),
    ])
    outs = place(outs, [
        (0, 0, 2, gx3), (1, 2, 0, uy3), (1, 0, 2, ux3), (0, 2, 0, gy3),
        (0, -1, -1, g11), (0, 1, -1, g12), (0, -1, 1, g21), (0, 1, 1, g22),
        (1, -1, -1, u11), (1, -1, 1, u12), (1, 1, -1, u21), (1, 1, 1, u22),
    ])
    outs = place(outs, [
        (0, -1, 2, g31), (0, 1, 2, g32), (1, 2, -1, u31), (1, 2, 1, u32),
    ])
    outs = place(outs, [
        (0, 2, -1, g13), (0, 2, 1, g23), (0, 2, 2, g33),
        (1, -1, 2, u13), (1, 1, 2, u23), (1, 2, 2, u33),
    ])
    return (*outs, column_gate, column_up)


def solution(mesh):
    return jax.shard_map(
        per_device,
        mesh=mesh,
        in_specs=(P("rows", "tp"),) * 6 + (P("rows"),),
        out_specs=(P(None, "tp"), P(None, "tp"), P("tp"), P("tp")),
        check_vma=False,
    )
```

```python
import jax
import jax.numpy as jnp
from jax import lax
from jax.experimental import pallas as pl
from jax.experimental.pallas import tpu as pltpu
from jax.sharding import PartitionSpec as P

learn_rate = 0.015
decay_rate = 0.1
tiny_value = 1e-08
SIDE = 4
TP = 16


def send(value, dy, dx):
    pairs = []
    for y in range(SIDE):
        for x in range(SIDE):
            for t in range(TP):
                s = 1 - 2 * (t % 2)
                to = ((y + s * dy) % SIDE) * SIDE + (x + s * dx) % SIDE
                pairs.append(((y * SIDE + x) * TP + t, to * TP + t))
    return lax.ppermute(value, ("rows", "tp"), pairs)


def place(outs, pieces, extra=()):
    blocks = [p[3] for p in pieces]
    rows = blocks[0].shape[0]

    def body(*refs):
        n = len(blocks)
        ins = refs[2 : 2 + n]
        dst = refs[2 + n + len(extra) : 4 + n + len(extra)]
        sems = refs[-1]
        r = lax.axis_index("rows")
        s = 1 - 2 * (lax.axis_index("tp") % 2)
        y, x = r // SIDE, r % SIDE
        copies = []
        for k, (which, dy, dx, _) in enumerate(pieces):
            at = ((y + s * dy + 2 * SIDE) % SIDE) * SIDE + (x + s * dx + 2 * SIDE) % SIDE
            copies.append(pltpu.make_async_copy(ins[k], dst[which].at[pl.ds(at * rows, rows), :], sems.at[k]))
        for c in copies:
            c.start()
        for c in copies:
            c.wait()

    any_spec = pl.BlockSpec(memory_space=pl.ANY)
    return pl.pallas_call(
        body,
        out_shape=tuple(jax.ShapeDtypeStruct(o.shape, o.dtype) for o in outs),
        in_specs=[any_spec] * 2 + [pl.BlockSpec(memory_space=pltpu.VMEM)] * len(blocks) + [any_spec] * len(extra),
        out_specs=(any_spec, any_spec),
        input_output_aliases={0: 0, 1: 1},
        scratch_shapes=[pltpu.SemaphoreType.DMA((len(blocks),))],
    )(*outs, *blocks, *extra)


def blank(shape, dtype):
    return pl.pallas_call(
        lambda a, b: None,
        out_shape=(jax.ShapeDtypeStruct(shape, dtype),) * 2,
        out_specs=(pl.BlockSpec(memory_space=pl.ANY),) * 2,
    )()


def max_over(v):
    c = jnp.broadcast_to(v, (SIDE * SIDE, v.shape[0]))
    return jnp.max(lax.all_to_all(c, "rows", 0, 0, tiled=True), axis=0)


def per_device(train_gate, drift_gate, spread_gate, train_up, drift_up, spread_up, norm_gain):
    whole_gate = train_gate - learn_rate * (
        drift_gate / (jnp.sqrt(spread_gate) + tiny_value) + decay_rate * train_gate
    )
    whole_up = train_up - learn_rate * (
        drift_up / (jnp.sqrt(spread_up) + tiny_value) + decay_rate * train_up
    )
    gained_gate = whole_gate * norm_gain[:, None]
    gained_up = whole_up * norm_gain[:, None]
    both = jnp.concatenate([jnp.max(jnp.abs(gained_gate), axis=0), jnp.max(jnp.abs(gained_up), axis=0)])
    both = max_over(both)
    width = train_gate.shape[1]
    column_gate, column_up = both[:width], both[width:]
    g = (gained_gate / column_gate).astype(jnp.bfloat16)
    u = (gained_up / column_up).astype(jnp.bfloat16)
    outs = blank((train_gate.shape[0] * SIDE * SIDE, width), jnp.bfloat16)

    gx1, uy1, gx2, uy2 = send(g, 0, 1), send(u, 1, 0), send(g, 0, -1), send(u, -1, 0)
    ux1, gy1, ux2, gy2 = send(u, 0, 1), send(g, 1, 0), send(u, 0, -1), send(g, -1, 0)
    gx3, uy3 = send(gx1, 0, 1), send(uy1, 1, 0)
    ux3, gy3 = send(ux2, 0, -1), send(gy2, -1, 0)
    g11, u11, g12, u12 = send(gx1, 1, 0), send(uy1, 0, 1), send(gx1, -1, 0), send(uy1, 0, -1)
    g21, u21, g22, u22 = send(gx2, 1, 0), send(uy2, 0, 1), send(gx2, -1, 0), send(uy2, 0, -1)
    g31, u31, g32, u32 = send(gx3, 1, 0), send(uy3, 0, 1), send(gx3, -1, 0), send(uy3, 0, -1)
    g13, u13 = send(g11, 1, 0), send(u11, 0, 1)
    g23, u23 = send(g22, -1, 0), send(u22, 0, -1)
    g33, u33 = send(g31, 1, 0), send(u31, 0, 1)

    outs = place(outs, [
        (0, 0, 0, g), (1, 0, 0, u),
        (0, 0, -1, gx1), (0, 0, 1, gx2), (1, -1, 0, uy1), (1, 1, 0, uy2),
        (1, 0, -1, ux1), (1, 0, 1, ux2), (0, -1, 0, gy1), (0, 1, 0, gy2),
    ])
    outs = place(outs, [
        (0, 0, 2, gx3), (1, 2, 0, uy3), (1, 0, 2, ux3), (0, 2, 0, gy3),
        (0, -1, -1, g11), (0, 1, -1, g12), (0, -1, 1, g21), (0, 1, 1, g22),
        (1, -1, -1, u11), (1, -1, 1, u12), (1, 1, -1, u21), (1, 1, 1, u22),
    ])
    outs = place(outs, [
        (0, -1, 2, g31), (0, 1, 2, g32), (1, 2, -1, u31), (1, 2, 1, u32),
    ])
    outs = place(outs, [
        (0, 2, -1, g13), (0, 2, 1, g23), (0, 2, 2, g33),
        (1, -1, 2, u13), (1, 1, 2, u23), (1, 2, 2, u33),
    ])
    return (*outs, column_gate, column_up)


def solution(mesh):
    return jax.shard_map(
        per_device,
        mesh=mesh,
        in_specs=(P("rows", "tp"),) * 6 + (P("rows"),),
        out_specs=(P(None, "tp"), P(None, "tp"), P("tp"), P("tp")),
        check_vma=False,
    )
```

```python
import jax
import jax.numpy as jnp
from jax import lax
from jax.experimental import pallas as pl
from jax.experimental.pallas import tpu as pltpu
from jax.sharding import PartitionSpec as P

learn_rate = 0.015
decay_rate = 0.1
tiny_value = 1e-08
SIDE = 4
TP = 16


def send(value, dy, dx):
    pairs = []
    for y in range(SIDE):
        for x in range(SIDE):
            for t in range(TP):
                s = 1 - 2 * (t % 2)
                to = ((y + s * dy) % SIDE) * SIDE + (x + s * dx) % SIDE
                pairs.append(((y * SIDE + x) * TP + t, to * TP + t))
    return lax.ppermute(value, ("rows", "tp"), pairs)


def place(outs, pieces):
    blocks = [pltpu.with_memory_space_constraint(p[3], pltpu.VMEM) for p in pieces]
    rows = outs[0].shape[0] // (SIDE * SIDE)

    def body(*refs):
        n = len(blocks)
        ins = refs[2 : 2 + n]
        dst = refs[2 + n : 4 + n]
        sems = refs[-1]
        r = lax.axis_index("rows")
        s = 1 - 2 * (lax.axis_index("tp") % 2)
        y, x = r // SIDE, r % SIDE
        copies = []
        for k, (which, dy, dx, block, first) in enumerate(pieces):
            at = ((y + s * dy + 2 * SIDE) % SIDE) * SIDE + (x + s * dx + 2 * SIDE) % SIDE
            there = pl.ds(at * rows + first, block.shape[0])
            copies.append(pltpu.make_async_copy(ins[k], dst[which].at[there, :], sems.at[k]))
        for c in copies:
            c.start()
        for c in copies:
            c.wait()

    any_spec = pl.BlockSpec(memory_space=pl.ANY)
    return pl.pallas_call(
        body,
        out_shape=tuple(jax.ShapeDtypeStruct(o.shape, o.dtype) for o in outs),
        in_specs=[any_spec] * (2 + len(blocks)),
        out_specs=(any_spec, any_spec),
        input_output_aliases={0: 0, 1: 1},
        scratch_shapes=[pltpu.SemaphoreType.DMA((len(blocks),))],
        compiler_params=pltpu.CompilerParams(vmem_limit_bytes=1 << 20),
    )(*outs, *blocks)


def blank(shape, dtype):
    return pl.pallas_call(
        lambda a, b: None,
        out_shape=(jax.ShapeDtypeStruct(shape, dtype),) * 2,
        out_specs=(pl.BlockSpec(memory_space=pl.ANY),) * 2,
        compiler_params=pltpu.CompilerParams(vmem_limit_bytes=1 << 20),
    )()


def stepped(train, drift, spread):
    return train - learn_rate * (drift / (jnp.sqrt(spread) + tiny_value) + decay_rate * train)


def coded(value, peak):
    part = value * (1.0 / peak)
    return lax.optimization_barrier((part * jnp.abs(part) * TOP).astype(jnp.float16))


def decoded(code, scale):
    code = code.astype(jnp.float32)
    return (code * lax.rsqrt(jnp.maximum(jnp.abs(code), SMALL)) * scale).astype(jnp.bfloat16)


SMALL = 1e-30
TOP = 32768.0

SLOTS = (
    (("gx1", "g", 0, 1), ("uy1", "u", 1, 0), ("ux1", "u", 0, 1), ("gy1", "g", 1, 0)),
    (("gx2", "g", 0, -1), ("uy2", "u", -1, 0), ("ux2", "u", 0, -1), ("gy2", "g", -1, 0)),
    (("gx3", "gx1", 0, 1), ("uy3", "uy1", 1, 0), ("u11", "uy1", 0, 1), ("g11", "gx1", 1, 0)),
    (("u22", "uy2", 0, -1), ("g22", "gx2", -1, 0), ("ux3", "ux2", 0, -1), ("gy3", "gy2", -1, 0)),
    (("u31", "uy3", 0, 1), ("g31", "gx3", 1, 0), ("u21", "uy2", 0, 1), ("g21", "gx2", 1, 0)),
    (("u32", "uy3", 0, -1), ("g32", "gx3", -1, 0), ("u23", "u22", 0, -1), ("g23", "g22", -1, 0)),
    (("u33", "u31", 0, 1), ("g33", "g31", 1, 0), ("u13", "u11", 0, 1), ("g13", "g11", 1, 0)),
    (("u12", "uy1", 0, -1), ("g12", "gx1", -1, 0)),
)
ROUTE = tuple(r for slot in SLOTS for r in slot)
ORIGIN = {"g": (0, 0), "u": (0, 0)}
BATCHES = [tuple(ORIGIN) + tuple(r[0] for r in SLOTS[0])] + [tuple(r[0] for r in slot) for slot in SLOTS[1:]]
for _name, _source, _dy, _dx in ROUTE:
    _y, _x = ORIGIN[_source]
    ORIGIN[_name] = (_y - _dy, _x - _dx)


def per_device(train_gate, drift_gate, spread_gate, train_up, drift_up, spread_up, norm_gain):
    rows, width = train_gate.shape
    gate = stepped(train_gate, drift_gate, spread_gate) * norm_gain[:, None]
    up = stepped(train_up, drift_up, spread_up) * norm_gain[:, None]
    peak_gate, peak_up = (jnp.maximum(jnp.max(jnp.abs(v), axis=0), SMALL) for v in (gate, up))
    have = {"g": coded(gate, peak_gate), "u": coded(up, peak_up)}
    peak = jnp.concatenate([peak_gate, peak_up])
    peaks = jnp.broadcast_to(peak, (SIDE * SIDE, 2 * width))
    peaks = lax.all_to_all(peaks, "rows", 0, 0, tiled=True)
    column = jnp.max(peaks, axis=0)
    column_gate, column_up = column[:width], column[width:]
    scales = peaks * (TOP**-0.5 / column)
    outs = blank((rows * SIDE * SIDE, width), jnp.bfloat16)
    for name, source, dy, dx in ROUTE:
        have[name] = send(have[source], dy, dx)
    at = lax.axis_index("rows")
    sense = 1 - 2 * (lax.axis_index("tp") % 2)

    def scale_of(name):
        dy, dx = ORIGIN[name]
        y = (at // SIDE + sense * dy + 2 * SIDE) % SIDE
        x = (at % SIDE + sense * dx + 2 * SIDE) % SIDE
        low = width * (name[0] == "u")
        return lax.dynamic_slice(scales, (y * SIDE + x, low), (1, width))

    for batch in BATCHES:
        pieces = [(int(n[0] == "u"), *ORIGIN[n], decoded(have[n], scale_of(n)), 0) for n in batch]
        outs = place(outs, pieces)
    return (*outs, column_gate, column_up)


def solution(mesh):
    return jax.shard_map(
        per_device,
        mesh=mesh,
        in_specs=(P("rows", "tp"),) * 6 + (P("rows"),),
        out_specs=(P(None, "tp"), P(None, "tp"), P("tp"), P("tp")),
        check_vma=False,
    )
```

```python
import jax
import jax.numpy as jnp
from jax import lax
from jax.experimental import pallas as pl
from jax.experimental.pallas import tpu as pltpu
from jax.sharding import PartitionSpec as P

learn_rate = 0.015
decay_rate = 0.1
tiny_value = 1e-08
SIDE = 4
TP = 16


def send(value, dy, dx):
    pairs = []
    for y in range(SIDE):
        for x in range(SIDE):
            for t in range(TP):
                s = 1 - 2 * (t % 2)
                to = ((y + s * dy) % SIDE) * SIDE + (x + s * dx) % SIDE
                pairs.append(((y * SIDE + x) * TP + t, to * TP + t))
    return lax.ppermute(value, ("rows", "tp"), pairs)


def place(outs, pieces):
    blocks = [pltpu.with_memory_space_constraint(p[3], pltpu.VMEM) for p in pieces]
    rows = outs[0].shape[0] // (SIDE * SIDE)

    def body(*refs):
        n = len(blocks)
        ins = refs[2 : 2 + n]
        dst = refs[2 + n : 4 + n]
        sems = refs[-1]
        r = lax.axis_index("rows")
        s = 1 - 2 * (lax.axis_index("tp") % 2)
        y, x = r // SIDE, r % SIDE
        copies = []
        for k, (which, dy, dx, block, first) in enumerate(pieces):
            at = ((y + s * dy + 2 * SIDE) % SIDE) * SIDE + (x + s * dx + 2 * SIDE) % SIDE
            there = pl.ds(at * rows + first, block.shape[0])
            copies.append(pltpu.make_async_copy(ins[k], dst[which].at[there, :], sems.at[k]))
        for c in copies:
            c.start()
        for c in copies:
            c.wait()

    any_spec = pl.BlockSpec(memory_space=pl.ANY)
    return pl.pallas_call(
        body,
        out_shape=tuple(jax.ShapeDtypeStruct(o.shape, o.dtype) for o in outs),
        in_specs=[any_spec] * (2 + len(blocks)),
        out_specs=(any_spec, any_spec),
        input_output_aliases={0: 0, 1: 1},
        scratch_shapes=[pltpu.SemaphoreType.DMA((len(blocks),))],
        compiler_params=pltpu.CompilerParams(vmem_limit_bytes=1 << 20),
    )(*outs, *blocks)


def blank(shape, dtype):
    return pl.pallas_call(
        lambda a, b: None,
        out_shape=(jax.ShapeDtypeStruct(shape, dtype),) * 2,
        out_specs=(pl.BlockSpec(memory_space=pl.ANY),) * 2,
        compiler_params=pltpu.CompilerParams(vmem_limit_bytes=1 << 20),
    )()


def stepped(train, drift, spread):
    return train - learn_rate * (drift / (jnp.sqrt(spread) + tiny_value) + decay_rate * train)


def coded(value, peak):
    part = value * (1.0 / peak)
    return lax.optimization_barrier((part * jnp.abs(part) * TOP).astype(jnp.float16))


def decoded(code, scale):
    code = code.astype(jnp.float32)
    return (code * lax.rsqrt(jnp.maximum(jnp.abs(code), SMALL)) * scale).astype(jnp.bfloat16)


SMALL = 1e-30
TOP = 32768.0

SLOTS = (
    (("gx1", "g", 0, 1), ("gy1", "g", 1, 0), ("ux1", "u", 0, 1), ("uy1", "u", 1, 0)),
    (("gx2", "g", 0, -1), ("uy2", "u", -1, 0)),
    (("ux2", "u", 0, -1), ("gy2", "g", -1, 0)),
    (("gx3", "gx1", 0, 1), ("uy3", "uy1", 1, 0), ("u11", "uy1", 0, 1), ("g11", "gx1", 1, 0)),
    (("u22", "uy2", 0, -1), ("g22", "gx2", -1, 0), ("ux3", "ux2", 0, -1), ("gy3", "gy2", -1, 0)),
    (("u31", "uy3", 0, 1), ("g31", "gx3", 1, 0), ("u21", "uy2", 0, 1), ("g21", "gx2", 1, 0)),
    (
        ("u13", "u11", 0, 1), ("g13", "g11", 1, 0),
        ("u32", "uy3", 0, -1), ("g32", "gx3", -1, 0), ("u12", "uy1", 0, -1), ("g12", "gx1", -1, 0),
    ),
    (("u23", "u22", 0, -1), ("g23", "g22", -1, 0), ("u33", "u31", 0, 1), ("g33", "g31", 1, 0)),
)
ROUTE = tuple(r for slot in SLOTS for r in slot)
ORIGIN = {"g": (0, 0), "u": (0, 0)}
_ARRIVE = [tuple(r[0] for r in slot) for slot in SLOTS]
BATCHES = [tuple(ORIGIN) + _ARRIVE[0], _ARRIVE[1] + _ARRIVE[2], *_ARRIVE[3:7], _ARRIVE[7][:2], _ARRIVE[7][2:]]
for _name, _source, _dy, _dx in ROUTE:
    _y, _x = ORIGIN[_source]
    ORIGIN[_name] = (_y - _dy, _x - _dx)


def per_device(train_gate, drift_gate, spread_gate, train_up, drift_up, spread_up, norm_gain):
    rows, width = train_gate.shape
    gate = stepped(train_gate, drift_gate, spread_gate) * norm_gain[:, None]
    peak_gate = jnp.maximum(jnp.max(jnp.abs(gate), axis=0), SMALL)
    have = {"g": coded(gate, peak_gate)}
    up = stepped(train_up, drift_up, spread_up) * norm_gain[:, None]
    peak_up = jnp.maximum(jnp.max(jnp.abs(up), axis=0), SMALL)
    have["u"] = coded(up, peak_up)
    peak = jnp.concatenate([peak_gate, peak_up])
    peaks = jnp.broadcast_to(peak, (SIDE * SIDE, 2 * width))
    peaks = lax.all_to_all(peaks, "rows", 0, 0, tiled=True)
    column = jnp.max(peaks, axis=0)
    column_gate, column_up = column[:width], column[width:]
    scales = peaks * (TOP**-0.5 / column)
    outs = blank((rows * SIDE * SIDE, width), jnp.bfloat16)
    for name, source, dy, dx in ROUTE:
        have[name] = send(have[source], dy, dx)
    at = lax.axis_index("rows")
    sense = 1 - 2 * (lax.axis_index("tp") % 2)

    def scale_of(name):
        dy, dx = ORIGIN[name]
        y = (at // SIDE + sense * dy + 2 * SIDE) % SIDE
        x = (at % SIDE + sense * dx + 2 * SIDE) % SIDE
        low = width * (name[0] == "u")
        return lax.dynamic_slice(scales, (y * SIDE + x, low), (1, width))

    for batch in BATCHES:
        pieces = [(int(n[0] == "u"), *ORIGIN[n], decoded(have[n], scale_of(n)), 0) for n in batch]
        outs = place(outs, pieces)
    return (*outs, column_gate, column_up)


def solution(mesh):
    return jax.shard_map(
        per_device,
        mesh=mesh,
        in_specs=(P("rows", "tp"),) * 6 + (P("rows"),),
        out_specs=(P(None, "tp"), P(None, "tp"), P("tp"), P("tp")),
        check_vma=False,
    )
```
